128 devices in a mesh: dp: 2 (over core), ep: 64 (over z, y, x).
Axes of the slice: x: 4, y: 4, z: 4, core: 2. Of those that a mesh axis runs over, the one named last changes fastest.
Arguments:
- x_tokens: bfloat16 [65536, 768], P(('dp', 'ep'))
- expert_id: int32 [65536], P(('dp', 'ep'))
- token_slot: int32 [65536], P(('dp', 'ep'))
- grad_y: bfloat16 [65536, 768], P(('dp', 'ep'))
- w_router: float32 [768, 64], replicated
- w_in: bfloat16 [64, 768, 3072], P('ep')
- w_out: bfloat16 [64, 3072, 768], P('ep')
- row_in: float32 [64, 768], P('ep')
- col_in: float32 [64, 3072], P('ep')
- row_out: float32 [64, 3072], P('ep')
- col_out: float32 [64, 768], P('ep')
- row_router: float32 [768], replicated
- col_router: float32 [64], replicated
Outputs:
- output 1: bfloat16 [64, 768, 3072], P('ep')
- output 2: bfloat16 [64, 3072, 768], P('ep')
- output 3: float32 [768, 64], replicated
- output 4: float32 [64, 768], P('ep')
- output 5: float32 [64, 3072], P('ep')
- output 6: float32 [64, 3072], P('ep')
- output 7: float32 [64, 768], P('ep')
- output 8: float32 [768], replicated
- output 9: float32 [64], replicated
- output 10: bfloat16 [65536, 768], P(('dp', 'ep'))
All inputs are finite; a program needn't handle non-finite values.
Results may differ from the reference program's by a relative error of at most 0.00445.
Values are sent between devices in bfloat16 or wider.
A program may use at most 1 GiB of HBM per device.

```python
import jax
import jax.numpy as jnp
from jax import lax
import math

GROUPS = 128
TOK = 512
D = 768
FF = 3072
E = 64
CAPACITY = 10
OPT_STEP = 2

DECAY_RATE = 1.0 - OPT_STEP ** -0.8
LR_BASE = min(0.01, 1.0 / math.sqrt(OPT_STEP))
AUX_COEF = 0.01
PRECISE = lax.Precision.HIGHEST


def draw_routing(base_key):
    key_hot, key_shift, key_rand = jax.random.split(base_key, 3)
    hot_id = jax.random.randint(key_hot, (GROUPS, 1), 0, E)
    shift_id = jax.random.randint(key_shift, (GROUPS, 1), 0, E)
    rand_ids = jax.random.randint(key_rand, (GROUPS, TOK), 0, E)
    position = jnp.arange(TOK)[None, :]
    spread = (position // 4 + shift_id) % E
    spread_row = (position % 4 == 1) & (position // 4 < E)
    expert_id = jnp.where(position % 4 == 0, hot_id, jnp.where(spread_row, spread, rand_ids))
    onehot = (expert_id[:, :, None] == jnp.arange(E)[None, None, :]).astype(jnp.int32)
    arrive_rank = jnp.sum(jnp.cumsum(onehot, axis=1) * onehot, axis=2) - 1
    token_slot = jnp.where(arrive_rank < CAPACITY, arrive_rank, -1)
    return expert_id.reshape(GROUPS * TOK).astype(jnp.int32), token_slot.reshape(GROUPS * TOK).astype(jnp.int32)


def draw_stat(stat_key, stat_shape, stat_scale):
    return stat_scale * jnp.exp(jax.random.uniform(stat_key, stat_shape, jnp.float32, -1.0, 1.0))


def setup_inputs(seed: int = 0) -> dict:
    sub_keys = jax.random.split(jax.random.key(seed), 12)
    all_tokens = GROUPS * TOK
    x_tokens = jax.random.normal(sub_keys[0], (all_tokens, D), jnp.float32).astype(jnp.bfloat16)
    grad_y = jax.random.normal(sub_keys[1], (all_tokens, D), jnp.float32).astype(jnp.bfloat16)
    expert_id, token_slot = draw_routing(sub_keys[2])
    w_router = jax.random.normal(sub_keys[3], (D, E), jnp.float32) * D ** -0.5
    w_in = (jax.random.normal(sub_keys[4], (E, D, FF), jnp.float32) * D ** -0.5).astype(jnp.bfloat16)
    w_out = (jax.random.normal(sub_keys[5], (E, FF, D), jnp.float32) * FF ** -0.5).astype(jnp.bfloat16)
    out_scale = 1.36 * GROUPS * TOK / E ** 3
    in_scale = out_scale * D / FF
    router_scale = out_scale * D
    return dict(x_tokens=x_tokens, expert_id=expert_id, token_slot=token_slot, grad_y=grad_y, w_router=w_router, w_in=w_in, w_out=w_out, row_in=draw_stat(sub_keys[6], (E, D), in_scale), col_in=draw_stat(sub_keys[7], (E, FF), in_scale), row_out=draw_stat(sub_keys[8], (E, FF), out_scale), col_out=draw_stat(sub_keys[9], (E, D), out_scale), row_router=draw_stat(sub_keys[10], (D,), router_scale), col_router=draw_stat(sub_keys[11], (E,), router_scale))


def gather_rows(table, index):
    return jax.vmap(lambda group_rows, group_index: jnp.take(group_rows, group_index, axis=0, mode='fill', fill_value=0))(table, index)


def slot_sources(flat_pos):
    return jnp.full((E * CAPACITY,), TOK, jnp.int32).at[flat_pos].set(jnp.arange(TOK, dtype=jnp.int32), mode='drop')


def optimizer_step(weight, gradient, row_stat, col_stat):
    grad_sq = gradient * gradient + 1e-30
    row_new = DECAY_RATE * row_stat + (1.0 - DECAY_RATE) * jnp.mean(grad_sq, axis=-1)
    col_new = DECAY_RATE * col_stat + (1.0 - DECAY_RATE) * jnp.mean(grad_sq, axis=-2)
    row_norm = row_new / jnp.mean(row_new, axis=-1, keepdims=True)
    update = gradient * lax.rsqrt(row_norm)[..., :, None] * lax.rsqrt(col_new)[..., None, :]
    upd_rms = jnp.sqrt(jnp.mean(update * update, axis=(-2, -1), keepdims=True))
    update = update / jnp.maximum(1.0, upd_rms)
    w_full = weight.astype(jnp.float32)
    w_rms = jnp.sqrt(jnp.mean(w_full * w_full, axis=(-2, -1), keepdims=True))
    new_weight = w_full - LR_BASE * jnp.maximum(1e-3, w_rms) * update
    return new_weight, row_new, col_new


def expert_step(operands):
    buf_x, buf_gh, win_e, wout_e = operands
    win_f = win_e.astype(jnp.float32)
    wout_f = wout_e.astype(jnp.float32)
    pre_act = jnp.einsum('gcd,df->gcf', buf_x.astype(jnp.float32), win_f).astype(jnp.bfloat16)
    hid_act = jnp.maximum(pre_act, 0)
    exp_out = jnp.einsum('gcf,fd->gcd', hid_act.astype(jnp.float32), wout_f).astype(jnp.bfloat16)
    grad_act = jnp.einsum('gcd,fd->gcf', buf_gh.astype(jnp.float32), wout_f)
    grad_pre = jnp.where(pre_act > 0, grad_act, 0.0).astype(jnp.bfloat16)
    grad_wout = jnp.einsum('gcf,gcd->fd', hid_act.astype(jnp.float32), buf_gh.astype(jnp.float32))
    grad_win = jnp.einsum('gcd,gcf->df', buf_x.astype(jnp.float32), grad_pre.astype(jnp.float32))
    grad_buf = jnp.einsum('gcf,df->gcd', grad_pre.astype(jnp.float32), win_f).astype(jnp.bfloat16)
    return exp_out, grad_buf, grad_win, grad_wout


def reference(x_tokens, expert_id, token_slot, grad_y, w_router, w_in, w_out, row_in, col_in, row_out, col_out, row_router, col_router):
    x_grp = x_tokens.reshape(GROUPS, TOK, D)
    dy_grp = grad_y.reshape(GROUPS, TOK, D)
    group_ids = expert_id.reshape(GROUPS, TOK)
    group_slots = token_slot.reshape(GROUPS, TOK)
    x_wide = x_grp.astype(jnp.float32)
    logits = jnp.einsum('gtd,de->gte', x_wide, w_router, precision=PRECISE)
    gate_probs = jax.nn.softmax(logits, axis=-1)
    onehot = (group_ids[:, :, None] == jnp.arange(E)[None, None, :]).astype(jnp.float32)
    gate_val = jnp.sum(gate_probs * onehot, axis=-1)
    flat_pos = jnp.where(group_slots >= 0, group_ids * CAPACITY + group_slots, E * CAPACITY)
    src_tok = jax.vmap(slot_sources)(flat_pos)
    send_x = gather_rows(x_grp, src_tok).reshape(GROUPS, E, CAPACITY, D)
    grad_h = (gate_val[:, :, None] * dy_grp.astype(jnp.float32)).astype(jnp.bfloat16)
    send_gh = gather_rows(grad_h, src_tok).reshape(GROUPS, E, CAPACITY, D)
    exp_out, grad_buf, grad_win, grad_wout = lax.map(expert_step, (jnp.swapaxes(send_x, 0, 1), jnp.swapaxes(send_gh, 0, 1), w_in, w_out))
    out_tok = gather_rows(jnp.swapaxes(exp_out, 0, 1).reshape(GROUPS, E * CAPACITY, D), flat_pos)
    dx_expert = gather_rows(jnp.swapaxes(grad_buf, 0, 1).reshape(GROUPS, E * CAPACITY, D), flat_pos)
    grad_gate = jnp.sum(dy_grp.astype(jnp.float32) * out_tok.astype(jnp.float32), axis=-1)
    route_frac = jnp.mean(onehot, axis=1, keepdims=True)
    grad_prob = onehot * grad_gate[:, :, None] + AUX_COEF * E * route_frac / TOK
    grad_logits = gate_probs * (grad_prob - jnp.sum(gate_probs * grad_prob, axis=-1, keepdims=True))
    grad_router = jnp.einsum('gtd,gte->de', x_wide, grad_logits, precision=PRECISE)
    grad_x = (dx_expert.astype(jnp.float32) + jnp.einsum('gte,de->gtd', grad_logits, w_router, precision=PRECISE)).astype(jnp.bfloat16)
    new_in, row_in_new, col_in_new = optimizer_step(w_in, grad_win, row_in, col_in)
    new_out, row_out_new, col_out_new = optimizer_step(w_out, grad_wout, row_out, col_out)
    new_router, row_router_new, col_router_new = optimizer_step(w_router, grad_router, row_router, col_router)
    return (new_in.astype(jnp.bfloat16), new_out.astype(jnp.bfloat16), new_router, row_in_new, col_in_new, row_out_new, col_out_new, row_router_new, col_router_new, grad_x.reshape(GROUPS * TOK, D))
```

```python
import functools
import math

import jax
import jax.numpy as jnp
from jax import lax
from jax.experimental import pallas as pl
from jax.experimental.pallas import tpu as pltpu
from jax.sharding import PartitionSpec as P

OPT_STEP = 2
DECAY = 1.0 - OPT_STEP ** -0.8
LR = min(0.01, 1.0 / math.sqrt(OPT_STEP))
AUX = 0.01
MESH = pl.DeviceIdType.MESH
VMEM = pltpu.VMEM
bf16 = jnp.bfloat16
f32 = jnp.float32

N = 64
T = 512
D = 768
F = 3072
H = F // 2
C = 10
R = N * C
J = C // 2
L = 128
FT = 512
DT = 256
BLOCKS = ((0, 3), (3, J))


def dot(a, b, ca, cb):
    return lax.dot_general(a, b, (((ca,), (cb,)), ((), ())), preferred_element_type=f32)


def split3(v):
    hi = v.astype(bf16)
    rest = v - hi.astype(f32)
    mid = rest.astype(bf16)
    return hi, mid, (rest - mid.astype(f32)).astype(bf16)


def probs(logits3):
    logits = (logits3[:, 2 * L:] + logits3[:, L:2 * L]) + logits3[:, :L]
    lane = lax.broadcasted_iota(jnp.int32, logits.shape, 1)
    logits = jnp.where(lane < N, logits, -jnp.inf)
    e = jnp.exp(logits - jnp.max(logits, axis=1, keepdims=True))
    return e / jnp.sum(e, axis=1, keepdims=True)


def tr(v):
    return jnp.swapaxes(v, 0, 1)


def mean1(v):
    return jnp.sum(v, axis=1, keepdims=True) * (1.0 / v.shape[1])


def total(v):
    return jnp.sum(jnp.sum(v, axis=0, keepdims=True), axis=1, keepdims=True)


def kernel(x_hbm, dy_hbm, eid_ref, slot_ref, wrt_ref, win_hbm, wout_hbm,
           rin_ref, cin_ref, rout_ref, cout_ref, rr_ref, cr_ref,
           win_new, wout_new, wrt_new, rin_new, cin_new, rout_new, cout_new, rr_new, cr_new, dx_ref,
           win, wout, xv, dyv, sx, sdy, rx, rdy, xb, dyb, hb, dhb, act, da, gout, gin,
           wr3, p_tok, oh_tok, t_oh, pe_scr, gs, gr, rs_s, rs_r, ag_s, ag_r, back,
           st_s, st_r, hs_s, hs_r, sem_l,
           xs_s, xs_r, ds_s, ds_r, gs_s, gs_r, bs_s, bs_r, rss, rsr, ags, agr, dps, dpr):
    me = lax.axis_index("ep")
    c = lax.axis_index("dp")
    oc = 1 - c
    my_h = pl.multiple_of(c * H, H)
    ot_h = pl.multiple_of(oc * H, H)
    halves = (ot_h, my_h)
    barrier = pltpu.get_barrier_semaphore()
    z, y, x = me // 16, (me // 4) % 4, me % 4
    along_x = [(x + k) % 4 for k in range(4)]

    def peers(act_on):
        for k in range(1, 4):
            act_on(z * 16 + y * 4 + along_x[k])

        def step(n, _):
            base = ((z + n // 4) % 4) * 16 + ((y + n % 4) % 4) * 4
            for k in range(4):
                act_on(base + along_x[k])
            return 0
        lax.fori_loop(1, 16, step, 0)

    peers(lambda p: pl.semaphore_signal(barrier, inc=1, device_id={"ep": p}, device_id_type=MESH))
    pl.semaphore_signal(barrier, inc=1, device_id={"dp": oc}, device_id_type=MESH)

    loads = [pltpu.make_async_copy(src, dst, sem_l.at[n]) for n, (src, dst) in enumerate(
        ((x_hbm, xv), (dy_hbm, dyv), (win_hbm.at[0], win), (wout_hbm.at[0], wout)))]
    for load in loads:
        load.start()

    def send_all(src, dst, s, r):
        def go(p):
            pltpu.make_async_remote_copy(src(p), dst(me), s, r, device_id={"ep": p}, device_id_type=MESH).start()
        peers(go)

    def done_all(src, dst, s, r):
        most = pl.ds(0, N - 1)
        return pltpu.make_async_remote_copy(src(most), dst(most), s, r, device_id={"ep": me}, device_id_type=MESH)

    def swap(src, dst, n):
        return pltpu.make_async_remote_copy(src, dst, dps.at[n], dpr.at[n], device_id={"dp": oc}, device_id_type=MESH)

    def lanes_of(ref, b):
        lo, hi = BLOCKS[b]
        return lambda p: ref.at[p, :, lo * D:hi * D]

    def rows_of(ref):
        return lambda p: ref.at[p]

    x_io = (rows_of(sx), rows_of(rx), xs_s, xs_r)
    dy_io = [(lanes_of(sdy, b), lanes_of(rdy, b), ds_s.at[b], ds_r.at[b]) for b in range(2)]
    bk_io = [(lanes_of(sx, b), lanes_of(back, b), bs_s.at[b], bs_r.at[b]) for b in range(2)]
    g_io = (rows_of(gs), rows_of(gr), gs_s, gs_r)
    rs_io = (rows_of(rs_s), rows_of(rs_r), rss, rsr)

    eid = eid_ref[...]
    slot = slot_ref[...]
    code = jnp.where(slot >= 0, (slot >> 1) * L + 2 * eid + (slot & 1), -1)

    def dispatch(rows_ref, out_ref):
        rows = rows_ref[...]
        for j in range(J):
            pick = (lax.broadcasted_iota(jnp.int32, (L, T), 0) + j * L == code).astype(f32).astype(bf16)
            out_ref[:, :, j * D:(j + 1) * D] = dot(pick, rows, 1, 0).astype(bf16).reshape(N, 2, D)

    loads[0].wait()
    dispatch(xv, sx)
    pl.semaphore_wait(barrier, N)
    send_all(*x_io)
    loads[1].wait()
    dispatch(dyv, sdy)
    wrt = wrt_ref[...]
    for n, part in enumerate(split3(wrt)):
        wr3[n * L:(n + 1) * L, :] = jnp.concatenate([part, jnp.zeros_like(part)], axis=0)
    p_tok[...] = probs(dot(xv[...], wr3[...], 1, 1))
    e_col = tr(jnp.broadcast_to(eid.astype(f32), (L, T)))
    code_col = tr(jnp.broadcast_to(code.astype(f32), (L, T)))
    lane_t = lax.broadcasted_iota(jnp.int32, (T, L), 1)
    oh_tok[...] = (lane_t.astype(f32) == e_col).astype(f32)
    for j in range(J):
        t_oh[:, j * L:(j + 1) * L] = (lane_t + j * L == code_col.astype(jnp.int32)).astype(f32).astype(bf16)

    def sum_sq(ref, rows):
        def step(n, acc):
            v = ref[pl.ds(pl.multiple_of(n * 32, 32), 32), :].astype(f32)
            return acc + v * v
        return total(lax.fori_loop(0, rows // 32, step, jnp.zeros((32, ref.shape[1]), f32)))

    loads[2].wait()
    win_rms = jnp.sqrt(sum_sq(win, D) * (1.0 / (D * F)))
    done_all(*x_io).wait_send()
    send_all(*dy_io[0])
    loads[3].wait()
    wout_rms = jnp.sqrt(sum_sq(wout, F) * (1.0 / (D * F)))
    wr_rms = jnp.sqrt(total(wrt * wrt) * (1.0 / (D * N)))

    done_all(*x_io).wait_recv()
    rx[pl.ds(me, 1)] = sx[pl.ds(me, 1)]
    for j in range(J):
        xb[0, j * L:(j + 1) * L, :] = rx[:, :, j * D:(j + 1) * D].reshape(L, D)
    sw_x = swap(xb.at[0], xb.at[1], 0)
    sw_x.start()
    for s in range(2):
        for n in range(H // FT):
            a = dot(xb[0], win[:, pl.ds(halves[s] + n * FT, FT)], 1, 0).astype(bf16)
            act[s, :, n * FT:(n + 1) * FT] = jnp.maximum(a, 0)
        if s == 0:
            sw_act = swap(act.at[0], act.at[2], 1)
            sw_act.start()
    done_all(*dy_io[0]).wait_send()
    send_all(*dy_io[1])
    pe = probs(dot(xb[0], wr3[...], 1, 1))
    lane_r = lax.broadcasted_iota(jnp.int32, (R, L), 1)
    pe_scr[...] = jnp.broadcast_to(jnp.sum(jnp.where(lane_r == me, pe, 0.0), axis=1, keepdims=True), (R, L))
    for n in range(D // DT):
        cols = slice(n * DT, (n + 1) * DT)
        h = dot(act[0], wout[pl.ds(ot_h, H), cols], 1, 0) + dot(act[1], wout[pl.ds(my_h, H), cols], 1, 0)
        hb[:, cols] = h.astype(bf16)

    lane = lax.broadcasted_iota(jnp.int32, (L, L), 1)
    odd = lax.broadcasted_iota(jnp.int32, (L, L), 0) & 1
    wide = jnp.zeros((L, L), f32)
    sw_dh, sw_da = [], []
    for b, (lo, hi) in enumerate(BLOCKS):
        rows = slice(lo * L, hi * L)
        done_all(*dy_io[b]).wait_recv()
        rdy[pl.ds(me, 1), :, lo * D:hi * D] = sdy[pl.ds(me, 1), :, lo * D:hi * D]
        for j in range(lo, hi):
            dyb[j * L:(j + 1) * L, :] = rdy[:, :, j * D:(j + 1) * D].reshape(L, D)
        for j in range(lo, hi):
            jr = slice(j * L, (j + 1) * L)
            g = jnp.zeros((L, L), f32)
            for n in range(D // L):
                cols = slice(n * L, (n + 1) * L)
                v = dyb[jr, cols].astype(f32)
                dhb[0, jr, cols] = (pe_scr[jr, :] * v).astype(bf16)
                g = g + v * hb[jr, cols].astype(f32)
            wide = jnp.where(lane == 2 * j + odd, jnp.sum(g, axis=1, keepdims=True), wide)
        sw_dh.append(swap(dhb.at[0, rows], dhb.at[1, rows], 2 + b))
        sw_dh[b].start()
        if b == 1:
            gs[...] = wide.reshape(N, 2, L)
            send_all(*g_io)
        for s in range(2):
            for n in range(H // FT):
                cols = slice(n * FT, (n + 1) * FT)
                v = dot(dhb[0, rows, :], wout[pl.ds(halves[s] + n * FT, FT), :], 1, 1)
                da[s, rows, cols] = jnp.where(act[s, rows, cols] > 0, v, 0.0).astype(bf16)
            if s == 0:
                sw_da.append(swap(da.at[0, rows], da.at[2, rows], 4 + b))
                sw_da[b].start()
        for n in range(D // DT):
            dr = slice(n * DT, (n + 1) * DT)
            v = (dot(da[0, rows, :], win[dr, pl.ds(ot_h, H)], 1, 1) + dot(da[1, rows, :], win[dr, pl.ds(my_h, H)], 1, 1)).astype(bf16)
            for j in range(lo, hi):
                sx[:, :, j * D + n * DT:j * D + (n + 1) * DT] = v[(j - lo) * L:(j - lo + 1) * L, :].reshape(N, 2, DT)
        send_all(*bk_io[b])

    sw_x.wait()
    sw_act.wait()
    sw_dh[0].wait()
    sw_dh[1].wait()
    col = jnp.zeros((8, D), f32)
    for n in range(H // FT):
        cols = slice(n * FT, (n + 1) * FT)
        v = dot(act[1:3, :, cols].reshape(2 * R, FT), dhb[...].reshape(2 * R, D), 0, 0)
        gout[cols, :] = v
        sq = v * v
        part = sum(sq[:, m * L:(m + 1) * L] for m in range(D // L))
        rsum = jnp.sum(tr(part), axis=0, keepdims=True)
        hs_s[0, :, cols] = DECAY * rout_ref[:, pl.ds(my_h + n * FT, FT)] + (1.0 - DECAY) * (rsum * (1.0 / D) + 1e-30)
        col = col + jnp.sum(sq.reshape(FT // 8, 8, D), axis=0)
    st_s[0] = jnp.broadcast_to(jnp.sum(col, axis=0, keepdims=True), (8, D))
    sw_c = swap(st_s.at[0], st_r.at[0], 6)
    sw_c.start()

    done_all(*g_io).wait_recv()
    gr[pl.ds(me, 1)] = gs[pl.ds(me, 1)]
    gsum = gr[:, 0, :] + gr[:, 1, :]
    onehot = oh_tok[...]
    ohb = onehot[:, :N].astype(bf16)
    ghi, gmid, glo = split3(gsum)
    gt = (dot(ohb, glo, 1, 0) + dot(ohb, gmid, 1, 0)) + dot(ohb, ghi, 1, 0)
    slot_col = tr(jnp.broadcast_to(slot_ref[...].astype(f32), (L, T)))
    gtok = jnp.sum(jnp.where(lane_t.astype(f32) == slot_col, gt, 0.0), axis=1, keepdims=True)
    frac = jnp.sum(onehot, axis=0, keepdims=True) * (1.0 / T)
    prob = p_tok[...]
    dprob = onehot * gtok + (AUX * N / T) * frac
    dlog = prob * (dprob - jnp.sum(prob * dprob, axis=1, keepdims=True))
    dhi, dmid, dlo = split3(dlog)
    xs = xv[...]
    dwr = (dot(dlo, xs, 0, 0) + dot(dmid, xs, 0, 0)) + dot(dhi, xs, 0, 0)
    rs_s[...] = dwr[:N].reshape(N, 1, D)
    send_all(*rs_io)

    sw_da[0].wait()
    sw_da[1].wait()

    def gin_tile(n, racc):
        cols = slice(n * FT, (n + 1) * FT)
        v = dot(xb[...].reshape(2 * R, D), da[1:3, :, cols].reshape(2 * R, FT), 0, 0)
        gin[:, cols] = v
        sq = v * v
        csum = jnp.sum(sq, axis=0, keepdims=True)
        hs_s[1, :, cols] = DECAY * cin_ref[:, pl.ds(my_h + n * FT, FT)] + (1.0 - DECAY) * (csum * (1.0 / D) + 1e-30)
        return racc + sum(sq[:, m * L:(m + 1) * L] for m in range(FT // L))

    racc = gin_tile(0, jnp.zeros((D, L), f32))

    sw_c.wait()
    ctot = st_s[0, 0:1, :] + st_r[0, 0:1, :]
    cout_n = DECAY * cout_ref[...] + (1.0 - DECAY) * (ctot * (1.0 / F) + 1e-30)
    cout_new[...] = cout_n
    mean_r = DECAY * mean1(rout_ref[...]) + (1.0 - DECAY) * (mean1(ctot) * (1.0 / F) + 1e-30)
    a_out = lax.rsqrt(hs_s[0] / mean_r)
    b_out = lax.rsqrt(cout_n)

    def scale(ref, a, b, rows, cols):
        usq = jnp.zeros((8, L), f32)
        for n in range(rows // L):
            sc = tr(jnp.broadcast_to(a[:, n * L:(n + 1) * L], (L, L)))
            for m in range(cols // L):
                lanes = slice(m * L, (m + 1) * L)
                u = ref[n * L:(n + 1) * L, lanes] * sc * b[:, lanes]
                ref[n * L:(n + 1) * L, lanes] = u
                usq = usq + jnp.sum((u * u).reshape(L // 8, 8, L), axis=0)
        return total(usq)

    st_s[2, :, :L] = jnp.broadcast_to(scale(gout, a_out, b_out, H, D), (8, L))
    sw_uo = swap(st_s.at[2, :, pl.ds(0, L)], st_r.at[2, :, pl.ds(0, L)], 8)
    sw_uo.start()
    racc = gin_tile(1, racc)
    sw_uo.wait()
    uso = st_s[2, 0:1, 0:1] + st_r[2, 0:1, 0:1]
    k_out = LR * jnp.maximum(1e-3, wout_rms) / jnp.maximum(1.0, jnp.sqrt(uso * (1.0 / (D * F))))
    for n in range(H // L):
        rows = pl.ds(my_h + n * L, L)
        wout_new[0, rows, :] = (wout[rows, :].astype(f32) - k_out * gout[n * L:(n + 1) * L, :]).astype(bf16)
    out_half = wout_new.at[0, pl.ds(my_h, H), :]
    sw_wo = swap(out_half, out_half, 9)
    sw_wo.start()
    done_all(*rs_io).wait_recv()
    rs_r[pl.ds(me, 1)] = rs_s[pl.ds(me, 1)]
    st_s[3] = jnp.broadcast_to(jnp.sum(rs_r[...], axis=0), (8, D))
    sw_r = swap(st_s.at[3], st_r.at[3], 10)
    sw_r.start()
    racc = gin_tile(2, racc)
    st_s[1] = jnp.broadcast_to(jnp.sum(tr(racc), axis=0, keepdims=True), (8, D))
    sw_ri = swap(st_s.at[1], st_r.at[1], 7)
    sw_ri.start()
    sw_hs = swap(hs_s, hs_r, 11)
    sw_hs.start()
    sw_r.wait()
    ag_s[...] = st_s[3, 0:1, :] + st_r[3, 0:1, :]
    send_all(lambda p: ag_s, lambda p: ag_r.at[p], ags, agr)
    w6 = jnp.concatenate([wr3[:L], wr3[L:2 * L], wr3[:L], wr3[L:2 * L], wr3[2 * L:], wr3[:L]], axis=0)
    d6 = jnp.concatenate([dhi, dhi, dmid, dmid, dhi, dlo], axis=1)
    dxr = dot(d6, w6, 1, 0)

    sw_ri.wait()
    rtot = st_s[1, 0:1, :] + st_r[1, 0:1, :]
    rin_n = DECAY * rin_ref[...] + (1.0 - DECAY) * (rtot * (1.0 / F) + 1e-30)
    rin_new[...] = rin_n
    a_in = lax.rsqrt(rin_n / mean1(rin_n))
    b_in = lax.rsqrt(hs_s[1])
    st_s[2, :, L:2 * L] = jnp.broadcast_to(scale(gin, a_in, b_in, D, H), (8, L))
    sw_ui = swap(st_s.at[2, :, pl.ds(L, L)], st_r.at[2, :, pl.ds(L, L)], 12)
    sw_ui.start()

    for b, (lo, hi) in enumerate(BLOCKS):
        done_all(*bk_io[b]).wait()
        back[pl.ds(me, 1), :, lo * D:hi * D] = sx[pl.ds(me, 1), :, lo * D:hi * D]
    for j in range(J):
        dyb[j * L:(j + 1) * L, :] = back[:, :, j * D:(j + 1) * D].reshape(L, D)
    dx_ref[...] = (dot(t_oh[...], dyb[...], 1, 0) + dxr).astype(bf16)

    sw_ui.wait()
    usi = st_s[2, 0:1, L:L + 1] + st_r[2, 0:1, L:L + 1]
    k_in = LR * jnp.maximum(1e-3, win_rms) / jnp.maximum(1.0, jnp.sqrt(usi * (1.0 / (D * F))))
    sw_wi = []
    for n in range(D // L):
        rows = slice(n * L, (n + 1) * L)
        win_new[0, rows, pl.ds(my_h, H)] = (win[rows, pl.ds(my_h, H)].astype(f32) - k_in * gin[rows, :]).astype(bf16)
        if n % 2 == 1:
            part = win_new.at[0, (n - 1) * L:(n + 1) * L, pl.ds(my_h, H)]
            sw_wi.append(swap(part, part, 13 + n // 2))
            sw_wi[-1].start()

    done_all(lambda p: ag_r.at[p], lambda p: ag_r.at[p], ags, agr).wait()
    ag_r[me] = ag_s[...]
    grt = ag_r[...].reshape(N, D)
    sq = grt * grt
    rr_n = DECAY * rr_ref[...] + (1.0 - DECAY) * (jnp.sum(sq, axis=0, keepdims=True) * (1.0 / N) + 1e-30)
    rr_new[...] = rr_n
    cmean = jnp.sum(sq, axis=1, keepdims=True) * (1.0 / D) + 1e-30
    cr_col = tr(jnp.broadcast_to(jnp.concatenate([cr_ref[...], jnp.ones((1, L - N), f32)], axis=1), (L, L)))[:N, 0:1]
    cr_n = DECAY * cr_col + (1.0 - DECAY) * cmean
    cr_new[...] = tr(jnp.broadcast_to(jnp.concatenate([cr_n, jnp.ones((L - N, 1), f32)], axis=0), (L, L)))[0:1, :N]
    u = grt * lax.rsqrt(rr_n / mean1(rr_n)) * lax.rsqrt(cr_n)
    urms = jnp.sqrt(total(u * u) * (1.0 / (D * N)))
    k_r = LR * jnp.maximum(1e-3, wr_rms) / jnp.maximum(1.0, urms)
    wrt_new[...] = wrt_ref[...] - k_r * u

    done_all(*dy_io[1]).wait_send()
    done_all(*g_io).wait_send()
    done_all(*rs_io).wait_send()
    sw_hs.wait()
    for ref, n in ((rout_new, 0), (cin_new, 1)):
        ref[:, pl.ds(my_h, H)] = hs_s[n]
        ref[:, pl.ds(ot_h, H)] = hs_r[n]
    sw_wo.wait()
    for cp in sw_wi:
        cp.wait()


def finish(*refs):
    n = len(refs) // 2
    sems = refs[-1]
    copies = [pltpu.make_async_copy(refs[k], refs[n + k], sems.at[k]) for k in range(n)]
    for copy in copies:
        copy.start()
    for copy in copies:
        copy.wait()


def solution(mesh):
    tok = P(("dp", "ep"))
    row = P(("dp", "ep"), None)
    exp = P("ep")
    full = P()
    dma = pltpu.SemaphoreType.DMA
    vm = pl.BlockSpec(memory_space=VMEM)
    hb = pl.BlockSpec(memory_space=pl.ANY)

    def local_step(x, eid, slot, dy, wr, win, wout, rin, cin, rout, cout, rr, cr):
        shapes = (((1, D, F), bf16), ((1, F, D), bf16), ((N, D), f32), ((1, D), f32), ((1, F), f32), ((1, F), f32),
                  ((1, D), f32), ((1, D), f32), ((1, N), f32), ((T, D), bf16))
        outs = pl.pallas_call(
            kernel,
            out_shape=tuple(VMEM(*s) for s in shapes),
            in_specs=[hb, hb, vm, vm, vm, hb, hb] + [vm] * 6,
            out_specs=(vm,) * 10,
            scratch_shapes=[
                VMEM((D, F), bf16), VMEM((F, D), bf16), VMEM((T, D), bf16), VMEM((T, D), bf16),
                VMEM((N, 2, J * D), bf16), VMEM((N, 2, J * D), bf16), VMEM((N, 2, J * D), bf16), VMEM((N, 2, J * D), bf16),
                VMEM((2, R, D), bf16), VMEM((R, D), bf16), VMEM((R, D), bf16), VMEM((2, R, D), bf16),
                VMEM((3, R, H), bf16), VMEM((3, R, H), bf16),
                VMEM((H, D), f32), VMEM((D, H), f32),
                VMEM((3 * L, D), bf16), VMEM((T, L), f32), VMEM((T, L), f32), VMEM((T, R), bf16),
                VMEM((R, L), f32), VMEM((N, 2, L), f32), VMEM((N, 2, L), f32),
                VMEM((N, 1, D), f32), VMEM((N, 1, D), f32), VMEM((1, D), f32), VMEM((N, 1, D), f32), VMEM((N, 2, J * D), bf16),
                VMEM((4, 8, D), f32), VMEM((4, 8, D), f32), VMEM((2, 1, H), f32), VMEM((2, 1, H), f32),
                dma((4,)),
                dma, dma, dma((2,)), dma((2,)), dma, dma, dma((2,)), dma((2,)), dma, dma, dma, dma, dma((16,)), dma((16,)),
            ],
            compiler_params=pltpu.CompilerParams(collective_id=1, has_side_effects=True, vmem_limit_bytes=52 * 2**20),
            name="expert_step",
        )(x, dy, eid.reshape(1, T), slot.reshape(1, T), wr.T, win, wout, rin, cin, rout, cout, rr.reshape(1, D), cr.reshape(1, N))
        outs = pl.pallas_call(
            finish,
            out_shape=tuple(jax.ShapeDtypeStruct(*s) for s in shapes),
            in_specs=[vm] * 10,
            out_specs=(hb,) * 10,
            scratch_shapes=[dma((10,))],
            compiler_params=pltpu.CompilerParams(vmem_limit_bytes=2**20),
            name="write_out",
        )(*outs)
        return outs[:2] + (outs[2].T,) + outs[3:7] + (outs[7].reshape(D), outs[8].reshape(N), outs[9])

    in_specs = (row, tok, tok, row, full, exp, exp, exp, exp, exp, exp, full, full)
    out_specs = (exp, exp, full, exp, exp, exp, exp, full, full, row)
    return jax.shard_map(local_step, mesh=mesh, in_specs=in_specs, out_specs=out_specs, check_vma=False)
```
